512 devices in a mesh: wide: 64 (over z_hi, y, core), narrow: 8 (over z_lo, x).
Axes of the slice: x: 4, y: 8, z: 8 (z_hi: 4, z_lo: 2; z = z_hi * 2 + z_lo), core: 2. Of those that a mesh axis runs over, the one named last changes fastest.
Arguments:
- concentrations: float32 [256, 512, 256], P('wide', 'narrow'), may hold values from 0.1 to 2
- wind_speeds: bfloat16 [2, 2, 512, 256], P(None, None, ('narrow', 'wide')), may hold values from -0.59765625 to 0.59765625
- rate_constants: float32 [768], replicated, may hold values from 0.05 to 1
- reactants: int32 [768, 2], replicated, may hold values from 0 to 255
- products: int32 [768, 2], replicated, may hold values from 0 to 255
Outputs:
- after_chemistry: float32 [256, 512, 256], P(None, ('narrow', 'wide'))
The draws below stay inside these ranges and needn't reach their ends.
Inputs may be any that keep to these rules, and one draw needn't show every extreme that they name: `reactants`: each entry is a species number. `products`: each entry is a species number.
All inputs are finite; a program needn't handle non-finite values.
Results may differ from the reference program's by a relative error of at most 0.0003.
Values may be sent and summed in bfloat16 or wider, within the bound.
No kernel may reach another device: no remote copies, remote signals or barrier semaphores. Data moves between devices by JAX's collectives and lax.ppermute only.
A program may use at most 64 MiB of HBM per device.

```python
import math
import jax
import jax.numpy as jnp
from jax import lax

S = 256
R = 768
NY = 256
SUB = 2
SECTIONS = 6
NX = 512
N_NARROW = 8


def place_ends(result, key, low, high):
    longest = result.shape.index(max(result.shape))
    spots = []
    for shift in (0, 1):
        where = [jax.random.randint(jax.random.fold_in(key, axis), (), 0, length) for axis, length in enumerate(result.shape)]
        where[longest] = (where[longest] + shift) % result.shape[longest]
        spots.append(tuple(where))
    return result.at[spots[0]].set(low).at[spots[1]].set(high)


def block_scale(own_key, extent, shards, smallest, high):
    def one(dim, blocks):
        steps = jax.random.uniform(jax.random.fold_in(jax.random.fold_in(own_key, 6), dim), (blocks,), jnp.float32, smallest / len(shards), high / len(shards))
        return jnp.repeat(jnp.exp(steps), extent[dim] // blocks).reshape((-1,) + (1,) * (len(extent) - dim - 1))

    gain = one(*shards[0])
    for cut in shards[1:]:
        gain = gain * one(*cut)
    return gain


def setup_inputs(seed: int = 0) -> dict:
    keys = jax.random.split(jax.random.key(seed), 6)
    return {
        "concentrations": jnp.clip(jnp.exp(math.log(2.0) - 2.9957323 * jax.random.uniform(keys[0], (S, NX, NY), jnp.float32) ** block_scale(keys[0], (S, NX, NY), ((0, 64), (1, 8)), -0.2, 0.2)), 0.1, 2.0),
        "wind_speeds": jnp.clip(jax.random.uniform(keys[1], (SUB, 2, NX, NY), jnp.float32, -0.59765625, 0.59765625) * block_scale(keys[1], (SUB, 2, NX, NY), ((2, 512),), -0.4, 0.0), -0.59765625, 0.59765625).astype(jnp.bfloat16),
        "rate_constants": jnp.clip(jnp.exp(jax.random.uniform(keys[2], (R,), jnp.float32, math.log(0.05), math.log(1.0))), 0.05, 1.0),
        "reactants": place_ends(jax.random.randint(keys[3], (R, 2), 0, S), jax.random.fold_in(keys[3], 1), 0, S - 1).astype(jnp.int32),
        "products": place_ends(jax.random.randint(keys[4], (R, 2), 0, S), jax.random.fold_in(keys[4], 1), 0, S - 1).astype(jnp.int32),
    }


DIFFUSION = 0.1
CHEM_STEP = 0.02


def take_range(array, begin_at, end_at, along):
    along = along % array.ndim
    index = [slice(None)] * array.ndim
    index[along] = slice(begin_at, end_at)
    return array[tuple(index)]


def minmod(first_jump, second_jump):
    return jnp.maximum(0.0, jnp.minimum(first_jump, second_jump)) + jnp.minimum(0.0, jnp.maximum(first_jump, second_jump))


def sweep_axis(extended, speeds, along, closed):
    length = extended.shape[along]
    speed_face = 0.5 * (take_range(speeds, 0, length - 1, along) + take_range(speeds, 1, length, along))
    jumps = take_range(extended, 1, length, along) - take_range(extended, 0, length - 1, along)
    slopes = minmod(take_range(jumps, 0, length - 2, along), take_range(jumps, 1, length - 1, along))
    inner_speed = take_range(speed_face, 1, length - 2, along)
    left_value = take_range(extended, 1, length - 2, along) + 0.5 * (1.0 - inner_speed) * take_range(slopes, 0, length - 3, along)
    right_value = take_range(extended, 2, length - 1, along) - 0.5 * (1.0 + inner_speed) * take_range(slopes, 1, length - 2, along)
    face_flux = inner_speed * jnp.where(inner_speed >= 0.0, left_value, right_value) - DIFFUSION * take_range(jumps, 1, length - 2, along)
    if closed:
        position = lax.broadcasted_iota(jnp.int32, face_flux.shape, along % face_flux.ndim)
        face_flux = jnp.where((position > 0) & (position < length - 4), face_flux, 0.0)
    return take_range(extended, 2, length - 2, along) - (take_range(face_flux, 1, length - 3, along) - take_range(face_flux, 0, length - 4, along))


def sweep_second(tracer, speeds):
    pad_tracer = [(0, 0)] * (tracer.ndim - 1) + [(2, 2)]
    pad_speeds = [(0, 0)] * (speeds.ndim - 1) + [(2, 2)]
    return sweep_axis(jnp.pad(tracer, pad_tracer, mode="edge"), jnp.pad(speeds, pad_speeds, mode="edge"), -1, True)


def periodic(array):
    return jnp.concatenate([array[..., -2:, :], array, array[..., :2, :]], axis=-2)


def reference(concentrations, wind_speeds, rate_constants, reactants, products):
    tracer = concentrations
    speeds = wind_speeds.astype(jnp.float32)
    for substep in range(SUB):
        tracer = sweep_axis(periodic(tracer), periodic(speeds[substep, 0]), -2, False)
        tracer = sweep_second(tracer, speeds[substep, 1])
    blocks = tracer.reshape(S, N_NARROW, (NX // N_NARROW) * NY).transpose(1, 0, 2)

    def react_block(cell_block):
        for section_index in range(SECTIONS):
            rate_values = rate_constants[:, None] * cell_block[reactants[:, 0]] * cell_block[reactants[:, 1]]
            tendency = jax.ops.segment_sum(rate_values, products[:, 0], num_segments=S)
            tendency = tendency + jax.ops.segment_sum(rate_values, products[:, 1], num_segments=S)
            tendency = tendency - jax.ops.segment_sum(rate_values, reactants[:, 0], num_segments=S)
            tendency = tendency - jax.ops.segment_sum(rate_values, reactants[:, 1], num_segments=S)
            cell_block = cell_block + CHEM_STEP * tendency
        return cell_block

    reacted = lax.map(react_block, blocks)
    return reacted.transpose(1, 0, 2).reshape(S, NX, NY)
```

```python
import jax
import jax.numpy as jnp
from jax import lax
from jax.experimental import pallas as pl
from jax.experimental.pallas import tpu as pltpu
from jax.sharding import PartitionSpec as P

S = 256
SUB = 2
SECTIONS = 6
DIFFUSION = 0.1
CHEM_STEP = 0.02
RIM = 4
SENT = jnp.float16


def minmod(first_jump, second_jump):
    return jnp.maximum(0.0, jnp.minimum(first_jump, second_jump)) + jnp.minimum(
        0.0, jnp.maximum(first_jump, second_jump)
    )


def face_flux(here, there, slope_here, slope_there, jump, speed):
    forward = speed >= 0.0
    value = jnp.where(forward, here, there)
    slope = jnp.where(forward, slope_here, slope_there)
    reach = jnp.where(forward, 0.5 - 0.5 * speed, -0.5 - 0.5 * speed)
    return speed * (value + reach * slope) - DIFFUSION * jump


def sweep_rows(rows, winds):
    count = len(rows)
    jumps = [rows[i + 1] - rows[i] for i in range(count - 1)]
    slopes = [None] + [minmod(jumps[i - 1], jumps[i]) for i in range(1, count - 1)]
    fluxes = [None] + [
        face_flux(
            rows[i], rows[i + 1], slopes[i], slopes[i + 1], jumps[i], 0.5 * (winds[i] + winds[i + 1])
        )
        for i in range(1, count - 2)
    ]
    return [rows[i] - (fluxes[i] - fluxes[i - 1]) for i in range(2, count - 2)]


def sweep_lanes(row, wind, last):
    lanes = row.shape[-1]
    axis = row.ndim - 1

    def ahead(x):
        return pltpu.roll(x, lanes - 1, axis)

    def behind(x):
        return pltpu.roll(x, 1, axis)

    there = ahead(row)
    jump = jnp.where(last, 0.0, there - row)
    slope = minmod(behind(jump), jump)
    speed = jnp.where(last, 0.0, 0.5 * (wind + ahead(wind)))
    flux = face_flux(row, there, slope, ahead(slope), jump, speed)
    return row - (flux - behind(flux))


def transport_kernel(own_ref, above_ref, below_ref, winds_ref, out_ref, ext_ref, speed_ref):
    rows, groups, lanes = own_ref.shape
    half = rows // 2
    count = half + 2 * RIM
    ext_ref[0:RIM, 0:groups] = above_ref[...]
    ext_ref[RIM:count, 0:groups] = own_ref[0 : half + RIM]
    ext_ref[0 : count - RIM, groups:] = own_ref[half - RIM : rows]
    ext_ref[count - RIM : count, groups:] = below_ref[...]
    upper = lax.broadcasted_iota(jnp.int32, (2 * groups, lanes), 0) < groups
    last = lax.broadcasted_iota(jnp.int32, (2 * groups, lanes), 1) == lanes - 1
    speed_ref[...] = winds_ref[...].astype(jnp.float32)

    def wind_row(plane, at):
        if at < RIM:
            row, place = rows - RIM + at, SUB * 2 + plane
        elif at < RIM + rows:
            row, place = at - RIM, plane
        else:
            row, place = at - RIM - rows, SUB * 2 + plane
        return jnp.broadcast_to(speed_ref[row, place : place + 1], (2 * groups, lanes))

    def wind(plane, at):
        return jnp.where(upper, wind_row(plane, at), wind_row(plane, at + half))

    field = [ext_ref[i] for i in range(count)]
    first = 0
    for substep in range(SUB):
        winds = [wind(2 * substep, first + i) for i in range(len(field))]
        field = sweep_rows(field, winds)
        first += 2
        field = [
            sweep_lanes(row, wind(2 * substep + 1, first + i), last) for i, row in enumerate(field)
        ]
    for i, row in enumerate(field):
        out_ref[i] = row[0:groups].astype(out_ref.dtype)
        out_ref[half + i] = row[groups:].astype(out_ref.dtype)


def transport(own, above, below, winds):
    rows, groups, lanes = own.shape
    return pl.pallas_call(
        transport_kernel,
        out_shape=jax.ShapeDtypeStruct(own.shape, jnp.float32),
        in_specs=[pl.BlockSpec(memory_space=pltpu.VMEM)] * 4,
        out_specs=pl.BlockSpec(memory_space=pltpu.VMEM),
        scratch_shapes=[
            pltpu.VMEM((rows // 2 + 2 * RIM, 2 * groups, lanes), jnp.float32),
            pltpu.VMEM(winds.shape, jnp.float32),
        ],
        cost_estimate=pl.CostEstimate(flops=4_000_000_000, bytes_accessed=600_000, transcendentals=0),
        name="transport",
    )(own, above, below, winds)


def tables_kernel(rates_ref, reactants_ref, products_ref, pick_ref, net_ref, rate_ref):
    count = rates_ref.shape[-1]
    ids = lax.broadcasted_iota(jnp.int32, (S, count), 0)

    def one_hot(ref, place):
        return jnp.where(ids == ref[place : place + 1, :], 1.0, 0.0)

    first, second = one_hot(reactants_ref, 0), one_hot(reactants_ref, 1)
    pick_ref[0:count] = first.T.astype(jnp.bfloat16)
    pick_ref[count:] = second.T.astype(jnp.bfloat16)
    net = one_hot(products_ref, 0) + one_hot(products_ref, 1) - first - second
    net_ref[...] = net.astype(jnp.bfloat16)
    rate_ref[...] = jnp.broadcast_to(rates_ref[...], (128, count)).T


def tables(rate_constants, reactants, products):
    count = rate_constants.shape[0]
    return pl.pallas_call(
        tables_kernel,
        out_shape=(
            jax.ShapeDtypeStruct((2 * count, S), jnp.bfloat16),
            jax.ShapeDtypeStruct((S, count), jnp.bfloat16),
            jax.ShapeDtypeStruct((count, 128), jnp.float32),
        ),
        in_specs=[pl.BlockSpec(memory_space=pltpu.VMEM)] * 3,
        out_specs=(pl.BlockSpec(memory_space=pltpu.VMEM),) * 3,
        cost_estimate=pl.CostEstimate(flops=4_000_000_000, bytes_accessed=2_000_000, transcendentals=0),
        name="tables",
    )(rate_constants.reshape(1, count), reactants.T, products.T)


def two_terms(x):
    high = x.astype(jnp.bfloat16)
    return high, (x - high.astype(jnp.float32)).astype(jnp.bfloat16)


def chemistry_kernel(cells_ref, pick_ref, net_ref, rate_ref, out_ref):
    count = net_ref.shape[1]
    chunk = 256
    cells = cells_ref[...].reshape(S, cells_ref.shape[-1]).astype(jnp.float32)

    def dot(a, b):
        return jnp.dot(a, b, preferred_element_type=jnp.float32)

    def section(_, cells):
        high, low = two_terms(cells)
        change = jnp.zeros_like(cells)
        for at in range(0, count, chunk):
            here, there = slice(at, at + chunk), slice(count + at, count + at + chunk)
            first = dot(pick_ref[here], high) + dot(pick_ref[here], low)
            second = dot(pick_ref[there], high) + dot(pick_ref[there], low)
            constant = rate_ref[here]
            rate = jnp.concatenate([constant, constant], 1) * first * second
            rate_high, rate_low = two_terms(rate)
            change = change + dot(net_ref[:, here], rate_high) + dot(net_ref[:, here], rate_low)
        return cells + CHEM_STEP * change

    cells = lax.fori_loop(0, SECTIONS, section, cells)
    out_ref[...] = cells.reshape(out_ref.shape)


def chemistry(cells, pick, net, rate):
    columns = cells.shape[-1]
    return pl.pallas_call(
        chemistry_kernel,
        out_shape=jax.ShapeDtypeStruct((S, 1, columns), jnp.float32),
        in_specs=[pl.BlockSpec(memory_space=pltpu.VMEM)] * 4,
        out_specs=pl.BlockSpec(memory_space=pltpu.VMEM),
        cost_estimate=pl.CostEstimate(flops=4_000_000_000, bytes_accessed=2_000_000, transcendentals=0),
        name="chemistry",
    )(cells, pick, net, rate)


def on_device(concentrations, wind_speeds, rate_constants, reactants, products):
    groups, _, columns = concentrations.shape
    wide, narrow = lax.axis_size("wide"), lax.axis_size("narrow")
    at_wide, at_narrow = lax.axis_index("wide"), lax.axis_index("narrow")
    above, below = (at_narrow - 1) % narrow, (at_narrow + 1) % narrow
    planes = wind_speeds.reshape(SUB * 2, columns)
    own = concentrations.swapaxes(0, 1)
    wind_row = planes.astype(jnp.float32)[None]
    down = jnp.concatenate([own[-RIM:], wind_row], 0)
    up = jnp.concatenate([own[:RIM], wind_row], 0)
    peers = lax.broadcasted_iota(jnp.int32, (narrow, 1, 1, 1), 0)
    rims = lax.all_to_all(jnp.where(peers == below, down[None], up[None]), "narrow", 0, 0, tiled=True)
    from_above = lax.dynamic_index_in_dim(rims, above, 0, False)
    from_below = lax.dynamic_index_in_dim(rims, below, 0, False)
    rim_row = jnp.where(at_wide < wide // 2, from_below[RIM], from_above[RIM]).astype(planes.dtype)
    sent = jnp.concatenate([planes, rim_row], 0)
    winds = lax.all_to_all(
        jnp.broadcast_to(sent[None], (wide, *sent.shape)), "wide", 0, 0, tiled=True
    )
    pick, net, rate = tables(rate_constants, reactants, products)
    moved = transport(own, from_above[:RIM], from_below[:RIM], winds)
    cells = lax.all_to_all(moved.astype(SENT), "wide", 0, 0, tiled=True)
    return chemistry(cells.astype(jnp.float32), pick, net, rate)


def solution(mesh):
    return jax.shard_map(
        on_device,
        mesh=mesh,
        in_specs=(
            P("wide", "narrow", None),
            P(None, None, ("narrow", "wide"), None),
            P(),
            P(),
            P(),
        ),
        out_specs=P(None, ("narrow", "wide"), None),
        check_vma=False,
    )
```

```python
import functools

import jax
import jax.numpy as jnp
from jax import lax
from jax.experimental import pallas as pl
from jax.experimental.pallas import tpu as pltpu
from jax.sharding import PartitionSpec as P

S = 256
SUB = 2
SECTIONS = 6
DIFFUSION = 0.1
CHEM_STEP = 0.02
RIM = 4
SENT = jnp.float16


def minmod(first_jump, second_jump):
    return jnp.maximum(0.0, jnp.minimum(first_jump, second_jump)) + jnp.minimum(
        0.0, jnp.maximum(first_jump, second_jump)
    )


def face_flux(here, there, slope_here, slope_there, jump, speed):
    forward = speed >= 0.0
    value = jnp.where(forward, here, there)
    slope = jnp.where(forward, slope_here, slope_there)
    reach = jnp.where(forward, 0.5 - 0.5 * speed, -0.5 - 0.5 * speed)
    return speed * (value + reach * slope) - DIFFUSION * jump


def sweep_rows(rows, speeds):
    count = len(rows)
    jumps = [rows[i + 1] - rows[i] for i in range(count - 1)]
    slopes = [None] + [minmod(jumps[i - 1], jumps[i]) for i in range(1, count - 1)]
    fluxes = [None] + [
        face_flux(rows[i], rows[i + 1], slopes[i], slopes[i + 1], jumps[i], speeds[i])
        for i in range(1, count - 2)
    ]
    return [rows[i] - (fluxes[i] - fluxes[i - 1]) for i in range(2, count - 2)]


def maps_kernel(pick_ref, shift_ref, face_ref, *, rows, groups, planes):
    half = rows // 2
    count = pick_ref.shape[1]
    sources = pick_ref.shape[2]
    lanes = shift_ref.shape[0]
    at = lax.broadcasted_iota(jnp.int32, (count, sources), 0)
    source = lax.broadcasted_iota(jnp.int32, (count, sources), 1)
    row = at // (2 * groups) + jnp.where(at % (2 * groups) < groups, 0, half)
    before, after = row < RIM, row >= RIM + rows
    place = row - RIM + jnp.where(before, rows, 0) - jnp.where(after, rows, 0)
    start = place * (2 * planes) + jnp.where(before | after, planes, 0)
    for plane in range(planes):
        weight = 1.0 if plane % 2 else 0.5
        pick_ref[plane] = jnp.where(source == start + plane, weight, 0.0).astype(jnp.bfloat16)
    here = lax.broadcasted_iota(jnp.int32, (lanes, lanes), 0)
    there = lax.broadcasted_iota(jnp.int32, (lanes, lanes), 1)
    for i, step in enumerate((-2, -1, 1, 2)):
        moved = jnp.clip(there + step, 0, lanes - 1)
        shift_ref[:, i * lanes : (i + 1) * lanes] = jnp.where(here == moved, 1.0, 0.0).astype(
            jnp.bfloat16
        )
    below = ((here == there) | (here == there - 1)) & (there > 0)
    above = ((here == there) | (here == there + 1)) & (there < lanes - 1)
    face_ref[:, :lanes] = jnp.where(below, 0.5, 0.0).astype(jnp.bfloat16)
    face_ref[:, lanes:] = jnp.where(above, 0.5, 0.0).astype(jnp.bfloat16)


def maps(rows, groups, lanes):
    planes = SUB * 2
    count = (rows // 2 + 2 * RIM) * 2 * groups
    return pl.pallas_call(
        functools.partial(maps_kernel, rows=rows, groups=groups, planes=planes),
        out_shape=(
            jax.ShapeDtypeStruct((planes, count, rows * planes * 2), jnp.bfloat16),
            jax.ShapeDtypeStruct((lanes, 4 * lanes), jnp.bfloat16),
            jax.ShapeDtypeStruct((lanes, 2 * lanes), jnp.bfloat16),
        ),
        out_specs=(pl.BlockSpec(memory_space=pltpu.VMEM),) * 3,
        cost_estimate=pl.CostEstimate(flops=2_000_000_000, bytes_accessed=2_000_000, transcendentals=0),
        compiler_params=pltpu.CompilerParams(vmem_limit_bytes=8 << 20),
        name="maps",
    )()


def matmul(a, b):
    return jnp.dot(a, b, preferred_element_type=jnp.float32)


def two_terms(x):
    high = x.astype(jnp.bfloat16)
    return high, (x - high.astype(jnp.float32)).astype(jnp.bfloat16)


def transport_kernel(
    own_ref, above_ref, below_ref, winds_ref, pick_ref, shift_ref, face_ref, out_ref,
    ext_ref, moved_ref, speed_ref,
):
    rows, groups, lanes = own_ref.shape
    tall = 2 * groups
    half = rows // 2
    count = half + 2 * RIM
    ext_ref[0:RIM, 0:groups] = above_ref[...]
    ext_ref[RIM:count, 0:groups] = own_ref[0 : half + RIM]
    ext_ref[0 : count - RIM, groups:] = own_ref[half - RIM : rows]
    ext_ref[count - RIM : count, groups:] = below_ref[...]
    winds = winds_ref[...].reshape(rows * tall, lanes)

    field = [ext_ref[i] for i in range(count)]
    first = 0
    for substep in range(SUB):
        low, high = first * tall, (first + len(field)) * tall
        halves = matmul(pick_ref[2 * substep, low:high], winds)
        speeds = [
            halves[i * tall : (i + 1) * tall] + halves[(i + 1) * tall : (i + 2) * tall]
            for i in range(len(field) - 1)
        ]
        field = sweep_rows(field, speeds)
        first += 2
        size = len(field) * tall
        low = first * tall
        across = matmul(pick_ref[2 * substep + 1, low : low + size], winds).astype(jnp.bfloat16)
        speed_ref[0:size] = matmul(across, face_ref[...])
        upper, lower = two_terms(jnp.concatenate(field, 0))
        moved_ref[0:size] = matmul(upper, shift_ref[...]) + matmul(lower, shift_ref[...])
        swept = []
        for i, row in enumerate(field):
            part = slice(i * tall, (i + 1) * tall)
            back2, back1, next1, next2 = (
                moved_ref[part, k * lanes : (k + 1) * lanes] for k in range(4)
            )
            jumps = [back1 - back2, row - back1, next1 - row, next2 - next1]
            slopes = [minmod(jumps[k], jumps[k + 1]) for k in range(3)]
            low_flux = face_flux(back1, row, slopes[0], slopes[1], jumps[1], speed_ref[part, :lanes])
            high_flux = face_flux(row, next1, slopes[1], slopes[2], jumps[2], speed_ref[part, lanes:])
            swept.append(row - (high_flux - low_flux))
        field = swept
    for i, row in enumerate(field):
        out_ref[i] = row[0:groups].astype(out_ref.dtype)
        out_ref[half + i] = row[groups:].astype(out_ref.dtype)


def transport(own, above, below, winds):
    rows, groups, lanes = own.shape
    tall = 2 * groups
    size = (rows // 2 + 2 * RIM) * tall
    constants = maps(rows, groups, lanes)
    return pl.pallas_call(
        transport_kernel,
        out_shape=jax.ShapeDtypeStruct(own.shape, jnp.float32),
        in_specs=[pl.BlockSpec(memory_space=pltpu.VMEM)] * 7,
        out_specs=pl.BlockSpec(memory_space=pltpu.VMEM),
        scratch_shapes=[
            pltpu.VMEM((rows // 2 + 2 * RIM, tall, lanes), jnp.float32),
            pltpu.VMEM((size, 4 * lanes), jnp.float32),
            pltpu.VMEM((size, 2 * lanes), jnp.float32),
        ],
        cost_estimate=pl.CostEstimate(flops=4_000_000_000, bytes_accessed=600_000, transcendentals=0),
        compiler_params=pltpu.CompilerParams(vmem_limit_bytes=16 << 20),
        name="transport",
    )(own, above, below, winds, *constants)


def tables_kernel(rates_ref, reactants_ref, products_ref, pick_ref, net_ref, rate_ref):
    count = rates_ref.shape[-1]
    ids = lax.broadcasted_iota(jnp.int32, (S, count), 0)

    def one_hot(ref, place):
        return jnp.where(ids == ref[place : place + 1, :], 1.0, 0.0)

    first, second = one_hot(reactants_ref, 0), one_hot(reactants_ref, 1)
    pick_ref[0:count] = first.T.astype(jnp.bfloat16)
    pick_ref[count:] = second.T.astype(jnp.bfloat16)
    net = one_hot(products_ref, 0) + one_hot(products_ref, 1) - first - second
    net_ref[...] = net.astype(jnp.bfloat16)
    rate_ref[...] = jnp.broadcast_to(rates_ref[...], (128, count)).T


def tables(rate_constants, reactants, products):
    count = rate_constants.shape[0]
    return pl.pallas_call(
        tables_kernel,
        out_shape=(
            jax.ShapeDtypeStruct((2 * count, S), jnp.bfloat16),
            jax.ShapeDtypeStruct((S, count), jnp.bfloat16),
            jax.ShapeDtypeStruct((count, 128), jnp.float32),
        ),
        in_specs=[pl.BlockSpec(memory_space=pltpu.VMEM)] * 3,
        out_specs=(pl.BlockSpec(memory_space=pltpu.VMEM),) * 3,
        cost_estimate=pl.CostEstimate(flops=4_000_000_000, bytes_accessed=2_000_000, transcendentals=0),
        compiler_params=pltpu.CompilerParams(vmem_limit_bytes=16 << 20),
        name="tables",
    )(rate_constants.reshape(1, count), reactants.T, products.T)


def chemistry_kernel(cells_ref, pick_ref, net_ref, rate_ref, out_ref):
    count = net_ref.shape[1]
    chunk = 256
    cells = cells_ref[...].reshape(S, cells_ref.shape[-1]).astype(jnp.float32)

    def section(_, cells):
        high, low = two_terms(cells)
        change = jnp.zeros_like(cells)
        for at in range(0, count, chunk):
            here, there = slice(at, at + chunk), slice(count + at, count + at + chunk)
            first = matmul(pick_ref[here], high) + matmul(pick_ref[here], low)
            second = matmul(pick_ref[there], high) + matmul(pick_ref[there], low)
            constant = rate_ref[here]
            rate = jnp.concatenate([constant, constant], 1) * first * second
            rate_high, rate_low = two_terms(rate)
            change = change + matmul(net_ref[:, here], rate_high) + matmul(net_ref[:, here], rate_low)
        return cells + CHEM_STEP * change

    cells = lax.fori_loop(0, SECTIONS, section, cells)
    out_ref[...] = cells.reshape(out_ref.shape)


def chemistry(cells, pick, net, rate):
    columns = cells.shape[-1]
    return pl.pallas_call(
        chemistry_kernel,
        out_shape=jax.ShapeDtypeStruct((S, 1, columns), jnp.float32),
        in_specs=[pl.BlockSpec(memory_space=pltpu.VMEM)] * 4,
        out_specs=pl.BlockSpec(memory_space=pltpu.VMEM),
        cost_estimate=pl.CostEstimate(flops=4_000_000_000, bytes_accessed=2_000_000, transcendentals=0),
        compiler_params=pltpu.CompilerParams(vmem_limit_bytes=16 << 20),
        name="chemistry",
    )(cells, pick, net, rate)


def on_device(concentrations, wind_speeds, rate_constants, reactants, products):
    groups, _, columns = concentrations.shape
    wide, narrow = lax.axis_size("wide"), lax.axis_size("narrow")
    at_wide, at_narrow = lax.axis_index("wide"), lax.axis_index("narrow")
    above, below = (at_narrow - 1) % narrow, (at_narrow + 1) % narrow
    planes = wind_speeds.reshape(SUB * 2, columns)
    own = concentrations.swapaxes(0, 1)
    wind_row = planes.astype(jnp.float32)[None]
    down = jnp.concatenate([own[-RIM:], wind_row], 0)
    up = jnp.concatenate([own[:RIM], wind_row], 0)
    peers = lax.broadcasted_iota(jnp.int32, (narrow, 1, 1, 1), 0)
    rims = lax.all_to_all(jnp.where(peers == below, down[None], up[None]), "narrow", 0, 0, tiled=True)
    from_above = lax.dynamic_index_in_dim(rims, above, 0, False)
    from_below = lax.dynamic_index_in_dim(rims, below, 0, False)
    rim_row = jnp.where(at_wide < wide // 2, from_below[RIM], from_above[RIM]).astype(planes.dtype)
    sent = jnp.concatenate([planes, rim_row], 0)
    winds = lax.all_to_all(
        jnp.broadcast_to(sent[None], (wide, *sent.shape)), "wide", 0, 0, tiled=True
    )
    pick, net, rate = tables(rate_constants, reactants, products)
    moved = transport(own, from_above[:RIM], from_below[:RIM], winds)
    cells = lax.all_to_all(moved.astype(SENT), "wide", 0, 0, tiled=True)
    return chemistry(cells.astype(jnp.float32), pick, net, rate)


def solution(mesh):
    return jax.shard_map(
        on_device,
        mesh=mesh,
        in_specs=(
            P("wide", "narrow", None),
            P(None, None, ("narrow", "wide"), None),
            P(),
            P(),
            P(),
        ),
        out_specs=P(None, ("narrow", "wide"), None),
        check_vma=False,
    )
```

```python
import functools

import jax
import jax.numpy as jnp
from jax import lax
from jax.experimental import pallas as pl
from jax.experimental.pallas import tpu as pltpu
from jax.sharding import PartitionSpec as P

S = 256
SUB = 2
SECTIONS = 6
DIFFUSION = 0.1
CHEM_STEP = 0.02
RIM = 4
SENT = jnp.float16


def minmod(first_jump, second_jump):
    return jnp.maximum(0.0, jnp.minimum(first_jump, second_jump)) + jnp.minimum(
        0.0, jnp.maximum(first_jump, second_jump)
    )


def face_flux(here, there, slope_here, slope_there, jump, speed):
    forward = speed >= 0.0
    value = jnp.where(forward, here, there)
    slope = jnp.where(forward, slope_here, slope_there)
    reach = jnp.where(forward, 0.5 - 0.5 * speed, -0.5 - 0.5 * speed)
    return speed * (value + reach * slope) - DIFFUSION * jump


def sweep_rows(rows, speeds):
    count = len(rows)
    jumps = [rows[i + 1] - rows[i] for i in range(count - 1)]
    slopes = [None] + [minmod(jumps[i - 1], jumps[i]) for i in range(1, count - 1)]
    fluxes = [None] + [
        face_flux(rows[i], rows[i + 1], slopes[i], slopes[i + 1], jumps[i], speeds[i])
        for i in range(1, count - 2)
    ]
    return [rows[i] - (fluxes[i] - fluxes[i - 1]) for i in range(2, count - 2)]


def maps_kernel(pick_ref, shift_ref, face_ref, *, rows, groups, planes):
    half = rows // 2
    count = pick_ref.shape[1]
    sources = pick_ref.shape[2]
    lanes = shift_ref.shape[0]
    at = lax.broadcasted_iota(jnp.int32, (count, sources), 0)
    source = lax.broadcasted_iota(jnp.int32, (count, sources), 1)
    start = (at // (2 * groups) + jnp.where(at % (2 * groups) < groups, 0, half)) * planes
    for plane in range(planes):
        weight = 1.0 if plane % 2 else 0.5
        pick_ref[plane] = jnp.where(source == start + plane, weight, 0.0).astype(jnp.bfloat16)
    here = lax.broadcasted_iota(jnp.int32, (lanes, lanes), 0)
    there = lax.broadcasted_iota(jnp.int32, (lanes, lanes), 1)
    for i, step in enumerate((-2, -1, 1, 2)):
        moved = jnp.clip(there + step, 0, lanes - 1)
        shift_ref[:, i * lanes : (i + 1) * lanes] = jnp.where(here == moved, 1.0, 0.0).astype(
            jnp.bfloat16
        )
    below = ((here == there) | (here == there - 1)) & (there > 0)
    above = ((here == there) | (here == there + 1)) & (there < lanes - 1)
    face_ref[:, :lanes] = jnp.where(below, 0.5, 0.0).astype(jnp.bfloat16)
    face_ref[:, lanes:] = jnp.where(above, 0.5, 0.0).astype(jnp.bfloat16)


def wind_depth(rows):
    return pl.cdiv((rows + 2 * RIM) * SUB * 2, 128) * 128


def maps(rows, groups, lanes):
    planes = SUB * 2
    count = (rows // 2 + 2 * RIM) * 2 * groups
    return pl.pallas_call(
        functools.partial(maps_kernel, rows=rows, groups=groups, planes=planes),
        out_shape=(
            jax.ShapeDtypeStruct((planes, count, wind_depth(rows)), jnp.bfloat16),
            jax.ShapeDtypeStruct((lanes, 4 * lanes), jnp.bfloat16),
            jax.ShapeDtypeStruct((lanes, 2 * lanes), jnp.bfloat16),
        ),
        out_specs=(pl.BlockSpec(memory_space=pltpu.VMEM),) * 3,
        cost_estimate=pl.CostEstimate(flops=2_000_000_000, bytes_accessed=2_000_000, transcendentals=0),
        compiler_params=pltpu.CompilerParams(vmem_limit_bytes=8 << 20),
        name="maps",
    )()


def matmul(a, b):
    return jnp.dot(a, b, preferred_element_type=jnp.float32)


def two_terms(x):
    high = x.astype(jnp.bfloat16)
    return high, (x - high.astype(jnp.float32)).astype(jnp.bfloat16)


def transport_kernel(
    own_ref, above_ref, below_ref, winds_ref, pick_ref, shift_ref, face_ref, out_ref,
    ext_ref, wind_ref, moved_ref, speed_ref,
):
    rows, groups, lanes = own_ref.shape
    planes = winds_ref.shape[1]
    tall = 2 * groups
    half = rows // 2
    count = half + 2 * RIM
    above, below = above_ref[...], below_ref[...]
    ext_ref[0:RIM, 0:groups] = above[:, :groups]
    ext_ref[RIM:count, 0:groups] = own_ref[0 : half + RIM]
    ext_ref[0 : count - RIM, groups:] = own_ref[half - RIM : rows]
    ext_ref[count - RIM : count, groups:] = below[:, :groups]
    rim, inner = RIM * planes, rows * planes

    def wind_rows(cells):
        return cells.astype(jnp.float32).reshape(-1, lanes).astype(jnp.bfloat16)

    wind_ref[0:rim] = wind_rows(above[:, groups:])
    wind_ref[rim : rim + inner] = wind_rows(winds_ref[...])
    wind_ref[rim + inner : 2 * rim + inner] = wind_rows(below[:, groups:])
    wind_ref[2 * rim + inner :] = jnp.zeros((wind_ref.shape[0] - 2 * rim - inner, lanes), jnp.bfloat16)
    winds = wind_ref[...]

    field = [ext_ref[i] for i in range(count)]
    first = 0
    for substep in range(SUB):
        low, high = first * tall, (first + len(field)) * tall
        halves = matmul(pick_ref[2 * substep, low:high], winds)
        speeds = [
            halves[i * tall : (i + 1) * tall] + halves[(i + 1) * tall : (i + 2) * tall]
            for i in range(len(field) - 1)
        ]
        field = sweep_rows(field, speeds)
        first += 2
        size = len(field) * tall
        low = first * tall
        across = matmul(pick_ref[2 * substep + 1, low : low + size], winds).astype(jnp.bfloat16)
        speed_ref[0:size] = matmul(across, face_ref[...])
        upper, lower = two_terms(jnp.concatenate(field, 0))
        moved_ref[0:size] = matmul(upper, shift_ref[...]) + matmul(lower, shift_ref[...])
        swept = []
        for i, row in enumerate(field):
            part = slice(i * tall, (i + 1) * tall)
            back2, back1, next1, next2 = (
                moved_ref[part, k * lanes : (k + 1) * lanes] for k in range(4)
            )
            jumps = [back1 - back2, row - back1, next1 - row, next2 - next1]
            slopes = [minmod(jumps[k], jumps[k + 1]) for k in range(3)]
            low_flux = face_flux(back1, row, slopes[0], slopes[1], jumps[1], speed_ref[part, :lanes])
            high_flux = face_flux(row, next1, slopes[1], slopes[2], jumps[2], speed_ref[part, lanes:])
            swept.append(row - (high_flux - low_flux))
        field = swept
    for i, row in enumerate(field):
        out_ref[i] = row[0:groups].astype(out_ref.dtype)
        out_ref[half + i] = row[groups:].astype(out_ref.dtype)


def transport(own, above, below, winds):
    rows, groups, lanes = own.shape
    tall = 2 * groups
    size = (rows // 2 + 2 * RIM) * tall
    constants = maps(rows, groups, lanes)
    return pl.pallas_call(
        transport_kernel,
        out_shape=jax.ShapeDtypeStruct(own.shape, jnp.float32),
        in_specs=[pl.BlockSpec(memory_space=pltpu.VMEM)] * 7,
        out_specs=pl.BlockSpec(memory_space=pltpu.VMEM),
        scratch_shapes=[
            pltpu.VMEM((rows // 2 + 2 * RIM, tall, lanes), jnp.float32),
            pltpu.VMEM((wind_depth(rows), lanes), jnp.bfloat16),
            pltpu.VMEM((size, 4 * lanes), jnp.float32),
            pltpu.VMEM((size, 2 * lanes), jnp.float32),
        ],
        cost_estimate=pl.CostEstimate(flops=4_000_000_000, bytes_accessed=600_000, transcendentals=0),
        compiler_params=pltpu.CompilerParams(vmem_limit_bytes=16 << 20),
        name="transport",
    )(own, above, below, winds, *constants)


def tables_kernel(rates_ref, reactants_ref, products_ref, pick_ref, net_ref, rate_ref):
    count = rates_ref.shape[-1]
    ids = lax.broadcasted_iota(jnp.int32, (S, count), 0)

    def one_hot(ref, place):
        return jnp.where(ids == ref[place : place + 1, :], 1.0, 0.0)

    first, second = one_hot(reactants_ref, 0), one_hot(reactants_ref, 1)
    pick_ref[0:count] = first.T.astype(jnp.bfloat16)
    pick_ref[count:] = second.T.astype(jnp.bfloat16)
    net = one_hot(products_ref, 0) + one_hot(products_ref, 1) - first - second
    net_ref[...] = net.astype(jnp.bfloat16)
    rate_ref[...] = jnp.broadcast_to(rates_ref[...], (128, count)).T


def tables(rate_constants, reactants, products):
    count = rate_constants.shape[0]
    return pl.pallas_call(
        tables_kernel,
        out_shape=(
            jax.ShapeDtypeStruct((2 * count, S), jnp.bfloat16),
            jax.ShapeDtypeStruct((S, count), jnp.bfloat16),
            jax.ShapeDtypeStruct((count, 128), jnp.float32),
        ),
        in_specs=[pl.BlockSpec(memory_space=pltpu.VMEM)] * 3,
        out_specs=(pl.BlockSpec(memory_space=pltpu.VMEM),) * 3,
        cost_estimate=pl.CostEstimate(flops=4_000_000_000, bytes_accessed=2_000_000, transcendentals=0),
        compiler_params=pltpu.CompilerParams(vmem_limit_bytes=16 << 20),
        name="tables",
    )(rate_constants.reshape(1, count), reactants.T, products.T)


def chemistry_kernel(cells_ref, pick_ref, net_ref, rate_ref, out_ref):
    count = net_ref.shape[1]
    chunk = 256
    cells = cells_ref[...].reshape(S, cells_ref.shape[-1]).astype(jnp.float32)

    def section(_, cells):
        high, low = two_terms(cells)
        change = jnp.zeros_like(cells)
        for at in range(0, count, chunk):
            here, there = slice(at, at + chunk), slice(count + at, count + at + chunk)
            first = matmul(pick_ref[here], high) + matmul(pick_ref[here], low)
            second = matmul(pick_ref[there], high) + matmul(pick_ref[there], low)
            constant = rate_ref[here]
            rate = jnp.concatenate([constant, constant], 1) * first * second
            rate_high, rate_low = two_terms(rate)
            change = change + matmul(net_ref[:, here], rate_high) + matmul(net_ref[:, here], rate_low)
        return cells + CHEM_STEP * change

    cells = lax.fori_loop(0, SECTIONS, section, cells)
    out_ref[...] = cells.reshape(out_ref.shape)


def chemistry(cells, pick, net, rate):
    columns = cells.shape[-1]
    return pl.pallas_call(
        chemistry_kernel,
        out_shape=jax.ShapeDtypeStruct((S, 1, columns), jnp.float32),
        in_specs=[pl.BlockSpec(memory_space=pltpu.VMEM)] * 4,
        out_specs=pl.BlockSpec(memory_space=pltpu.VMEM),
        cost_estimate=pl.CostEstimate(flops=4_000_000_000, bytes_accessed=2_000_000, transcendentals=0),
        compiler_params=pltpu.CompilerParams(vmem_limit_bytes=16 << 20),
        name="chemistry",
    )(cells, pick, net, rate)


def on_device(concentrations, wind_speeds, rate_constants, reactants, products):
    groups, _, columns = concentrations.shape
    wide, narrow = lax.axis_size("wide"), lax.axis_size("narrow")
    winds = lax.all_to_all(
        jnp.broadcast_to(wind_speeds[None], (wide, *wind_speeds.shape)), "wide", 0, 0, tiled=True
    ).reshape(wide, SUB * 2, columns)
    own = concentrations.swapaxes(0, 1)

    def rim(part):
        return jnp.concatenate([own[part], winds[part].astype(jnp.float32)], 1)

    down = [(i, (i + 1) % narrow) for i in range(narrow)]
    from_above = lax.ppermute(rim(slice(-RIM, None)), "narrow", down)
    from_below = lax.ppermute(rim(slice(RIM)), "narrow", [(j, i) for i, j in down])
    pick, net, rate = tables(rate_constants, reactants, products)
    moved = transport(own, from_above, from_below, winds)
    cells = lax.all_to_all(moved.astype(SENT), "wide", 0, 0, tiled=True)
    return chemistry(cells.astype(jnp.float32), pick, net, rate)


def solution(mesh):
    return jax.shard_map(
        on_device,
        mesh=mesh,
        in_specs=(
            P("wide", "narrow", None),
            P(None, None, ("narrow", "wide"), None),
            P(),
            P(),
            P(),
        ),
        out_specs=P(None, ("narrow", "wide"), None),
        check_vma=False,
    )
```

```python
import functools

import jax
import jax.numpy as jnp
from jax import lax
from jax.experimental import pallas as pl
from jax.experimental.pallas import tpu as pltpu
from jax.sharding import PartitionSpec as P

S = 256
SUB = 2
SECTIONS = 6
DIFFUSION = 0.1
CHEM_STEP = 0.02
RIM = 4
SENT = jnp.float16


def minmod(first_jump, second_jump):
    return jnp.maximum(0.0, jnp.minimum(first_jump, second_jump)) + jnp.minimum(
        0.0, jnp.maximum(first_jump, second_jump)
    )


def face_flux(here, there, slope_here, slope_there, jump, speed):
    forward = speed >= 0.0
    value = jnp.where(forward, here, there)
    slope = jnp.where(forward, slope_here, slope_there)
    reach = jnp.where(forward, 0.5 - 0.5 * speed, -0.5 - 0.5 * speed)
    return speed * (value + reach * slope) - DIFFUSION * jump


def sweep_rows(rows, speeds):
    count = len(rows)
    jumps = [rows[i + 1] - rows[i] for i in range(count - 1)]
    slopes = [None] + [minmod(jumps[i - 1], jumps[i]) for i in range(1, count - 1)]
    fluxes = [None] + [
        face_flux(rows[i], rows[i + 1], slopes[i], slopes[i + 1], jumps[i], speeds[i])
        for i in range(1, count - 2)
    ]
    return [rows[i] - (fluxes[i] - fluxes[i - 1]) for i in range(2, count - 2)]


def maps_kernel(pick_ref, shift_ref, face_ref, *, rows, groups, planes):
    half = rows // 2
    count = pick_ref.shape[1]
    sources = pick_ref.shape[2]
    lanes = shift_ref.shape[0]
    at = lax.broadcasted_iota(jnp.int32, (count, sources), 0)
    source = lax.broadcasted_iota(jnp.int32, (count, sources), 1)
    start = (at // (2 * groups) + jnp.where(at % (2 * groups) < groups, 0, half)) * planes
    for plane in range(planes):
        weight = 1.0 if plane % 2 else 0.5
        pick_ref[plane] = jnp.where(source == start + plane, weight, 0.0).astype(jnp.bfloat16)
    here = lax.broadcasted_iota(jnp.int32, (lanes, lanes), 0)
    there = lax.broadcasted_iota(jnp.int32, (lanes, lanes), 1)
    for i, step in enumerate((-2, -1, 1, 2)):
        moved = jnp.clip(there + step, 0, lanes - 1)
        shift_ref[:, i * lanes : (i + 1) * lanes] = jnp.where(here == moved, 1.0, 0.0).astype(
            jnp.bfloat16
        )
    below = ((here == there) | (here == there - 1)) & (there > 0)
    above = ((here == there) | (here == there + 1)) & (there < lanes - 1)
    face_ref[:, :lanes] = jnp.where(below, 0.5, 0.0).astype(jnp.bfloat16)
    face_ref[:, lanes:] = jnp.where(above, 0.5, 0.0).astype(jnp.bfloat16)


def wind_depth(rows):
    return pl.cdiv((rows + 2 * RIM) * SUB * 2, 128) * 128


def maps(rows, groups, lanes):
    planes = SUB * 2
    count = (rows // 2 + 2 * RIM) * 2 * groups
    return pl.pallas_call(
        functools.partial(maps_kernel, rows=rows, groups=groups, planes=planes),
        out_shape=(
            jax.ShapeDtypeStruct((planes, count, wind_depth(rows)), jnp.bfloat16),
            jax.ShapeDtypeStruct((lanes, 4 * lanes), jnp.bfloat16),
            jax.ShapeDtypeStruct((lanes, 2 * lanes), jnp.bfloat16),
        ),
        out_specs=(pl.BlockSpec(memory_space=pltpu.VMEM),) * 3,
        cost_estimate=pl.CostEstimate(flops=2_000_000_000, bytes_accessed=2_000_000, transcendentals=0),
        compiler_params=pltpu.CompilerParams(vmem_limit_bytes=8 << 20),
        name="maps",
    )()


def matmul(a, b):
    return jnp.dot(a, b, preferred_element_type=jnp.float32)


def two_terms(x):
    high = x.astype(jnp.bfloat16)
    return high, (x - high.astype(jnp.float32)).astype(jnp.bfloat16)


def transport_kernel(
    own_ref, above_ref, below_ref, winds_ref, pick_ref, shift_ref, face_ref, out_ref,
    ext_ref, wind_ref, moved_ref, speed_ref,
):
    rows, groups, lanes = own_ref.shape
    planes = winds_ref.shape[1]
    tall = 2 * groups
    half = rows // 2
    count = half + 2 * RIM
    above, below = above_ref[...], below_ref[...]
    ext_ref[0:RIM, 0:groups] = above[:, :groups]
    ext_ref[RIM:count, 0:groups] = own_ref[0 : half + RIM]
    ext_ref[0 : count - RIM, groups:] = own_ref[half - RIM : rows]
    ext_ref[count - RIM : count, groups:] = below[:, :groups]
    rim, inner = RIM * planes, rows * planes

    def wind_rows(cells):
        return cells.astype(jnp.float32).reshape(-1, lanes).astype(jnp.bfloat16)

    wind_ref[0:rim] = wind_rows(above[:, groups:])
    wind_ref[rim : rim + inner] = wind_rows(winds_ref[...])
    wind_ref[rim + inner : 2 * rim + inner] = wind_rows(below[:, groups:])
    wind_ref[2 * rim + inner :] = jnp.zeros((wind_ref.shape[0] - 2 * rim - inner, lanes), jnp.bfloat16)
    winds = wind_ref[...]

    field = [ext_ref[i] for i in range(count)]
    first = 0
    for substep in range(SUB):
        low, high = first * tall, (first + len(field)) * tall
        halves = matmul(pick_ref[2 * substep, low:high], winds)
        speeds = [
            halves[i * tall : (i + 1) * tall] + halves[(i + 1) * tall : (i + 2) * tall]
            for i in range(len(field) - 1)
        ]
        field = sweep_rows(field, speeds)
        first += 2
        size = len(field) * tall
        low = first * tall
        across = matmul(pick_ref[2 * substep + 1, low : low + size], winds).astype(jnp.bfloat16)
        speed_ref[0:size] = matmul(across, face_ref[...])
        upper, lower = two_terms(jnp.concatenate(field, 0))
        moved_ref[0:size] = matmul(upper, shift_ref[...]) + matmul(lower, shift_ref[...])
        swept = []
        for i, row in enumerate(field):
            part = slice(i * tall, (i + 1) * tall)
            back2, back1, next1, next2 = (
                moved_ref[part, k * lanes : (k + 1) * lanes] for k in range(4)
            )
            jumps = [back1 - back2, row - back1, next1 - row, next2 - next1]
            slopes = [minmod(jumps[k], jumps[k + 1]) for k in range(3)]
            low_flux = face_flux(back1, row, slopes[0], slopes[1], jumps[1], speed_ref[part, :lanes])
            high_flux = face_flux(row, next1, slopes[1], slopes[2], jumps[2], speed_ref[part, lanes:])
            swept.append(row - (high_flux - low_flux))
        field = swept
    for i, row in enumerate(field):
        out_ref[i] = row[0:groups].astype(out_ref.dtype)
        out_ref[half + i] = row[groups:].astype(out_ref.dtype)


def transport(own, above, below, winds):
    rows, groups, lanes = own.shape
    tall = 2 * groups
    size = (rows // 2 + 2 * RIM) * tall
    constants = maps(rows, groups, lanes)
    return pl.pallas_call(
        transport_kernel,
        out_shape=jax.ShapeDtypeStruct(own.shape, jnp.float32),
        in_specs=[pl.BlockSpec(memory_space=pltpu.VMEM)] * 7,
        out_specs=pl.BlockSpec(memory_space=pltpu.VMEM),
        scratch_shapes=[
            pltpu.VMEM((rows // 2 + 2 * RIM, tall, lanes), jnp.float32),
            pltpu.VMEM((wind_depth(rows), lanes), jnp.bfloat16),
            pltpu.VMEM((size, 4 * lanes), jnp.float32),
            pltpu.VMEM((size, 2 * lanes), jnp.float32),
        ],
        cost_estimate=pl.CostEstimate(flops=4_000_000_000, bytes_accessed=600_000, transcendentals=0),
        compiler_params=pltpu.CompilerParams(vmem_limit_bytes=16 << 20),
        name="transport",
    )(own, above, below, winds, *constants)


def tables_kernel(reactants_ref, products_ref, pick_ref, net_ref):
    count = reactants_ref.shape[-1]
    ids = lax.broadcasted_iota(jnp.int32, (S, count), 0)

    def one_hot(ref, place):
        return jnp.where(ids == ref[place : place + 1, :], 1.0, 0.0)

    first, second = one_hot(reactants_ref, 0), one_hot(reactants_ref, 1)
    pick_ref[:, 0:count] = first.astype(jnp.bfloat16)
    pick_ref[:, count:] = second.astype(jnp.bfloat16)
    net = one_hot(products_ref, 0) + one_hot(products_ref, 1) - first - second
    net_ref[...] = net.T.astype(jnp.bfloat16)


def tables(rate_constants, reactants, products):
    count = rate_constants.shape[0]
    made = pl.pallas_call(
        tables_kernel,
        out_shape=(
            jax.ShapeDtypeStruct((S, 2 * count), jnp.bfloat16),
            jax.ShapeDtypeStruct((count, S), jnp.bfloat16),
        ),
        in_specs=[pl.BlockSpec(memory_space=pltpu.VMEM)] * 2,
        out_specs=(pl.BlockSpec(memory_space=pltpu.VMEM),) * 2,
        cost_estimate=pl.CostEstimate(flops=4_000_000_000, bytes_accessed=2_000_000, transcendentals=0),
        compiler_params=pltpu.CompilerParams(vmem_limit_bytes=16 << 20),
        name="tables",
    )(reactants.T, products.T)
    return *made, rate_constants.reshape(1, count)


def chemistry_kernel(cells_ref, pick_ref, net_ref, rate_ref, out_ref):
    count = net_ref.shape[0]
    chunk = 256
    cells = cells_ref[...].reshape(S, cells_ref.shape[-1]).astype(jnp.float32).T

    def picked(cells):
        high, low = two_terms(cells)
        return [
            matmul(high, pick_ref[:, at : at + chunk]) + matmul(low, pick_ref[:, at : at + chunk])
            for at in range(0, 2 * count, chunk)
        ]

    def reacted(cells, found):
        change = jnp.zeros_like(cells)
        for i, at in enumerate(range(0, count, chunk)):
            here = slice(at, at + chunk)
            pair = found[i] * found[i + count // chunk]
            rate_high, rate_low = two_terms(rate_ref[:, here] * pair)
            change = change + matmul(rate_high, net_ref[here]) + matmul(rate_low, net_ref[here])
        return cells + CHEM_STEP * change

    size = cells.shape[0] // 2
    early, late = cells[:size], cells[size:]
    found_late = picked(late)
    for section in range(SECTIONS):
        found_early = picked(early)
        late = reacted(late, found_late)
        early = reacted(early, found_early)
        if section < SECTIONS - 1:
            found_late = picked(late)
    out_ref[...] = jnp.concatenate([early, late], 0).T.reshape(out_ref.shape)


def chemistry(cells, pick, net, rate):
    columns = cells.shape[-1]
    return pl.pallas_call(
        chemistry_kernel,
        out_shape=jax.ShapeDtypeStruct((S, 1, columns), jnp.float32),
        in_specs=[pl.BlockSpec(memory_space=pltpu.VMEM)] * 4,
        out_specs=pl.BlockSpec(memory_space=pltpu.VMEM),
        cost_estimate=pl.CostEstimate(flops=4_000_000_000, bytes_accessed=2_000_000, transcendentals=0),
        compiler_params=pltpu.CompilerParams(vmem_limit_bytes=16 << 20),
        name="chemistry",
    )(cells, pick, net, rate)


def on_device(concentrations, wind_speeds, rate_constants, reactants, products):
    groups, _, columns = concentrations.shape
    wide, narrow = lax.axis_size("wide"), lax.axis_size("narrow")
    winds = lax.all_to_all(
        jnp.broadcast_to(wind_speeds[None], (wide, *wind_speeds.shape)), "wide", 0, 0, tiled=True
    ).reshape(wide, SUB * 2, columns)
    own = concentrations.swapaxes(0, 1)

    def rim(part):
        return jnp.concatenate([own[part], winds[part].astype(jnp.float32)], 1)

    down = [(i, (i + 1) % narrow) for i in range(narrow)]
    from_above = lax.ppermute(rim(slice(-RIM, None)), "narrow", down)
    from_below = lax.ppermute(rim(slice(RIM)), "narrow", [(j, i) for i, j in down])
    pick, net, rate = tables(rate_constants, reactants, products)
    moved = transport(own, from_above, from_below, winds)
    cells = lax.all_to_all(moved.astype(SENT), "wide", 0, 0, tiled=True)
    return chemistry(cells.astype(jnp.float32), pick, net, rate)


def solution(mesh):
    return jax.shard_map(
        on_device,
        mesh=mesh,
        in_specs=(
            P("wide", "narrow", None),
            P(None, None, ("narrow", "wide"), None),
            P(),
            P(),
            P(),
        ),
        out_specs=P(None, ("narrow", "wide"), None),
        check_vma=False,
    )
```

```python
import jax
import jax.numpy as jnp
from jax import lax
from jax.experimental import pallas as pl
from jax.experimental.pallas import tpu as pltpu
from jax.sharding import PartitionSpec as P


S = 256
SUB = 2
SECTIONS = 6
DIFFUSION = 0.1
CHEM_STEP = 0.02
RIM = 4
SENT = jnp.float16


def minmod(first_jump, second_jump):
    return jnp.maximum(0.0, jnp.minimum(first_jump, second_jump)) + jnp.minimum(
        0.0, jnp.maximum(first_jump, second_jump)
    )


def face_flux(here, there, slope_here, slope_there, jump, speed):
    forward = speed >= 0.0
    value = jnp.where(forward, here, there)
    slope = jnp.where(forward, slope_here, slope_there)
    reach = jnp.where(forward, 0.5 - 0.5 * speed, -0.5 - 0.5 * speed)
    return speed * (value + reach * slope) - DIFFUSION * jump


def sweep_rows(rows, speeds):
    count = len(rows)
    jumps = [rows[i + 1] - rows[i] for i in range(count - 1)]
    slopes = [None] + [minmod(jumps[i - 1], jumps[i]) for i in range(1, count - 1)]
    fluxes = [None] + [
        face_flux(rows[i], rows[i + 1], slopes[i], slopes[i + 1], jumps[i], speeds[i])
        for i in range(1, count - 2)
    ]
    return [rows[i] - (fluxes[i] - fluxes[i - 1]) for i in range(2, count - 2)]


def maps_kernel(shift_ref, face_ref):
    lanes = shift_ref.shape[0]
    here = lax.broadcasted_iota(jnp.int32, (lanes, lanes), 0)
    there = lax.broadcasted_iota(jnp.int32, (lanes, lanes), 1)
    for i, step in enumerate((-2, -1, 1, 2)):
        moved = jnp.clip(there + step, 0, lanes - 1)
        shift_ref[:, i * lanes : (i + 1) * lanes] = jnp.where(here == moved, 1.0, 0.0).astype(
            jnp.bfloat16
        )
    below = ((here == there) | (here == there - 1)) & (there > 0)
    above = ((here == there) | (here == there + 1)) & (there < lanes - 1)
    face_ref[:, :lanes] = jnp.where(below, 0.5, 0.0).astype(jnp.bfloat16)
    face_ref[:, lanes:] = jnp.where(above, 0.5, 0.0).astype(jnp.bfloat16)


def maps(lanes):
    return pl.pallas_call(
        maps_kernel,
        out_shape=(
            jax.ShapeDtypeStruct((lanes, 4 * lanes), jnp.bfloat16),
            jax.ShapeDtypeStruct((lanes, 2 * lanes), jnp.bfloat16),
        ),
        out_specs=(pl.BlockSpec(memory_space=pltpu.VMEM),) * 2,
        cost_estimate=pl.CostEstimate(flops=2_000_000_000, bytes_accessed=1_000_000, transcendentals=0),
        compiler_params=pltpu.CompilerParams(vmem_limit_bytes=8 << 20),
        name="maps",
    )()


def matmul(a, b):
    return jnp.dot(a, b, preferred_element_type=jnp.float32)


def two_terms(x):
    high = x.astype(jnp.bfloat16)
    return high, (x - high.astype(jnp.float32)).astype(jnp.bfloat16)


def transport_kernel(
    own_ref, above_ref, below_ref, winds_ref, shift_ref, face_ref, out_ref,
    ext_ref, wind_ref, moved_ref, speed_ref,
):
    rows, groups, lanes = own_ref.shape
    planes = winds_ref.shape[1]
    tall = 2 * groups
    half = rows // 2
    count = half + 2 * RIM
    above, below = above_ref[...], below_ref[...]
    ext_ref[0:RIM, 0:groups] = above[:, :groups]
    ext_ref[RIM:count, 0:groups] = own_ref[0 : half + RIM]
    ext_ref[0 : count - RIM, groups:] = own_ref[half - RIM : rows]
    ext_ref[count - RIM : count, groups:] = below[:, :groups]
    rim, inner = RIM * planes, rows * planes

    wind_ref[0:rim] = above[:, groups:].reshape(rim, lanes)
    wind_ref[rim : rim + inner] = winds_ref[...].astype(jnp.float32).reshape(inner, lanes)
    wind_ref[rim + inner :] = below[:, groups:].reshape(rim, lanes)
    speed_ref[...] = matmul(wind_ref[...].astype(jnp.bfloat16), face_ref[...])
    is_upper = lax.broadcasted_iota(jnp.int32, (tall, lanes), 0) < groups

    def spread(ref, plane, at, columns):
        here, there = (
            jnp.broadcast_to(ref[row : row + 1, columns], (tall, lanes))
            for row in (at * planes + plane, (at + half) * planes + plane)
        )
        return jnp.where(is_upper, here, there)

    field = [ext_ref[i] for i in range(count)]
    first = 0
    for substep in range(SUB):
        along = [
            spread(wind_ref, 2 * substep, first + i, slice(0, lanes)) for i in range(len(field))
        ]
        speeds = [0.5 * (along[i] + along[i + 1]) for i in range(len(field) - 1)]
        field = sweep_rows(field, speeds)
        first += 2
        size = len(field) * tall
        upper, lower = two_terms(jnp.concatenate(field, 0))
        moved_ref[0:size] = matmul(upper, shift_ref[...]) + matmul(lower, shift_ref[...])
        swept = []
        for i, row in enumerate(field):
            part = slice(i * tall, (i + 1) * tall)
            back2, back1, next1, next2 = (
                moved_ref[part, k * lanes : (k + 1) * lanes] for k in range(4)
            )
            jumps = [back1 - back2, row - back1, next1 - row, next2 - next1]
            slopes = [minmod(jumps[k], jumps[k + 1]) for k in range(3)]
            low_speed, high_speed = (
                spread(speed_ref, 2 * substep + 1, first + i, slice(k * lanes, (k + 1) * lanes))
                for k in range(2)
            )
            low_flux = face_flux(back1, row, slopes[0], slopes[1], jumps[1], low_speed)
            high_flux = face_flux(row, next1, slopes[1], slopes[2], jumps[2], high_speed)
            swept.append(row - (high_flux - low_flux))
        field = swept
    for i, row in enumerate(field):
        out_ref[i] = row[0:groups].astype(out_ref.dtype)
        out_ref[half + i] = row[groups:].astype(out_ref.dtype)


def transport(own, above, below, winds, *constants):
    rows, groups, lanes = own.shape
    tall = 2 * groups
    size = (rows // 2 + 2 * RIM) * tall
    depth = (rows + 2 * RIM) * winds.shape[1]
    return pl.pallas_call(
        transport_kernel,
        out_shape=jax.ShapeDtypeStruct(own.shape, jnp.float32),
        in_specs=[pl.BlockSpec(memory_space=pltpu.VMEM)] * 6,
        out_specs=pl.BlockSpec(memory_space=pltpu.VMEM),
        scratch_shapes=[
            pltpu.VMEM((rows // 2 + 2 * RIM, tall, lanes), jnp.float32),
            pltpu.VMEM((depth, lanes), jnp.float32),
            pltpu.VMEM((size, 4 * lanes), jnp.float32),
            pltpu.VMEM((depth, 2 * lanes), jnp.float32),
        ],
        cost_estimate=pl.CostEstimate(flops=4_000_000_000, bytes_accessed=600_000, transcendentals=0),
        compiler_params=pltpu.CompilerParams(vmem_limit_bytes=16 << 20),
        name="transport",
    )(own, above, below, winds, *constants)


def tables_kernel(reactants_ref, products_ref, pick_ref, net_ref):
    count = reactants_ref.shape[-1]
    ids = lax.broadcasted_iota(jnp.int32, (S, count), 0)

    def one_hot(ref, place):
        return jnp.where(ids == ref[place : place + 1, :], 1.0, 0.0)

    first, second = one_hot(reactants_ref, 0), one_hot(reactants_ref, 1)
    pick_ref[:, 0:count] = first.astype(jnp.bfloat16)
    pick_ref[:, count:] = second.astype(jnp.bfloat16)
    net = one_hot(products_ref, 0) + one_hot(products_ref, 1) - first - second
    net_ref[...] = net.T.astype(jnp.bfloat16)


def tables(rate_constants, reactants, products):
    count = rate_constants.shape[0]
    made = pl.pallas_call(
        tables_kernel,
        out_shape=(
            jax.ShapeDtypeStruct((S, 2 * count), jnp.bfloat16),
            jax.ShapeDtypeStruct((count, S), jnp.bfloat16),
        ),
        in_specs=[pl.BlockSpec(memory_space=pltpu.VMEM)] * 2,
        out_specs=(pl.BlockSpec(memory_space=pltpu.VMEM),) * 2,
        cost_estimate=pl.CostEstimate(flops=4_000_000_000, bytes_accessed=2_000_000, transcendentals=0),
        compiler_params=pltpu.CompilerParams(vmem_limit_bytes=16 << 20),
        name="tables",
    )(reactants.T, products.T)
    return *made, rate_constants.reshape(1, count)


def chemistry_kernel(cells_ref, pick_ref, net_ref, rate_ref, out_ref):
    count = net_ref.shape[0]
    chunk = 256
    cells = cells_ref[...].reshape(S, cells_ref.shape[-1]).astype(jnp.float32).T

    def picked(cells):
        high, low = two_terms(cells)
        return [
            matmul(high, pick_ref[:, at : at + chunk]) + matmul(low, pick_ref[:, at : at + chunk])
            for at in range(0, 2 * count, chunk)
        ]

    def reacted(cells, found):
        change = jnp.zeros_like(cells)
        for i, at in enumerate(range(0, count, chunk)):
            here = slice(at, at + chunk)
            pair = found[i] * found[i + count // chunk]
            rate_high, rate_low = two_terms(rate_ref[:, here] * pair)
            change = change + matmul(rate_high, net_ref[here]) + matmul(rate_low, net_ref[here])
        return cells + CHEM_STEP * change

    size = cells.shape[0] // 2
    early, late = cells[:size], cells[size:]
    found_late = picked(late)
    for section in range(SECTIONS):
        found_early = picked(early)
        late = reacted(late, found_late)
        early = reacted(early, found_early)
        if section < SECTIONS - 1:
            found_late = picked(late)
    out_ref[...] = jnp.concatenate([early, late], 0).T.reshape(out_ref.shape)


def chemistry(cells, pick, net, rate):
    columns = cells.shape[-1]
    return pl.pallas_call(
        chemistry_kernel,
        out_shape=jax.ShapeDtypeStruct((S, 1, columns), jnp.float32),
        in_specs=[pl.BlockSpec(memory_space=pltpu.VMEM)] * 4,
        out_specs=pl.BlockSpec(memory_space=pltpu.VMEM),
        cost_estimate=pl.CostEstimate(flops=4_000_000_000, bytes_accessed=2_000_000, transcendentals=0),
        compiler_params=pltpu.CompilerParams(vmem_limit_bytes=16 << 20),
        name="chemistry",
    )(cells, pick, net, rate)


def on_device(concentrations, wind_speeds, rate_constants, reactants, products):
    _, _, columns = concentrations.shape
    wide, narrow = lax.axis_size("wide"), lax.axis_size("narrow")
    winds = lax.all_to_all(
        jnp.broadcast_to(wind_speeds[None], (wide, *wind_speeds.shape)), "wide", 0, 0, tiled=True
    ).reshape(wide, SUB * 2, columns)
    moves = maps(columns)
    own = concentrations.swapaxes(0, 1)

    def rim(part):
        return jnp.concatenate([own[part], winds[part].astype(jnp.float32)], 1)

    down = [(i, (i + 1) % narrow) for i in range(narrow)]
    from_above = lax.ppermute(rim(slice(-RIM, None)), "narrow", down)
    from_below = lax.ppermute(rim(slice(RIM)), "narrow", [(j, i) for i, j in down])
    pick, net, rate = tables(rate_constants, reactants, products)
    moved = transport(own, from_above, from_below, winds, *moves)
    cells = lax.all_to_all(moved.astype(SENT), "wide", 0, 0, tiled=True)
    return chemistry(cells.astype(jnp.float32), pick, net, rate)


def solution(mesh):
    return jax.shard_map(
        on_device,
        mesh=mesh,
        in_specs=(
            P("wide", "narrow", None),
            P(None, None, ("narrow", "wide"), None),
            P(),
            P(),
            P(),
        ),
        out_specs=P(None, ("narrow", "wide"), None),
        check_vma=False,
    )
```

```python
import jax
import jax.numpy as jnp
from jax import lax
from jax.experimental import pallas as pl
from jax.experimental.pallas import tpu as pltpu
from jax.sharding import PartitionSpec as P


S = 256
SUB = 2
SECTIONS = 6
DIFFUSION = 0.1
CHEM_STEP = 0.02
RIM = 4
SENT = jnp.float16


def minmod(first_jump, second_jump):
    return jnp.maximum(0.0, jnp.minimum(first_jump, second_jump)) + jnp.minimum(
        0.0, jnp.maximum(first_jump, second_jump)
    )


def face_flux(here, there, slope_here, slope_there, jump, speed):
    forward = speed >= 0.0
    value = jnp.where(forward, here, there)
    slope = jnp.where(forward, slope_here, slope_there)
    reach = jnp.where(forward, 0.5 - 0.5 * speed, -0.5 - 0.5 * speed)
    return speed * (value + reach * slope) - DIFFUSION * jump


def sweep_rows(rows, speeds):
    count = len(rows)
    jumps = [rows[i + 1] - rows[i] for i in range(count - 1)]
    slopes = [None] + [minmod(jumps[i - 1], jumps[i]) for i in range(1, count - 1)]
    fluxes = [None] + [
        face_flux(rows[i], rows[i + 1], slopes[i], slopes[i + 1], jumps[i], speeds[i])
        for i in range(1, count - 2)
    ]
    return [rows[i] - (fluxes[i] - fluxes[i - 1]) for i in range(2, count - 2)]


def maps_kernel(shift_ref, face_ref):
    lanes = shift_ref.shape[0]
    here = lax.broadcasted_iota(jnp.int32, (lanes, lanes), 0)
    there = lax.broadcasted_iota(jnp.int32, (lanes, lanes), 1)
    for i, step in enumerate((-2, -1, 1, 2)):
        moved = jnp.clip(there + step, 0, lanes - 1)
        shift_ref[:, i * lanes : (i + 1) * lanes] = jnp.where(here == moved, 1.0, 0.0).astype(
            jnp.bfloat16
        )
    below = ((here == there) | (here == there - 1)) & (there > 0)
    above = ((here == there) | (here == there + 1)) & (there < lanes - 1)
    face_ref[:, :lanes] = jnp.where(below, 0.5, 0.0).astype(jnp.bfloat16)
    face_ref[:, lanes:] = jnp.where(above, 0.5, 0.0).astype(jnp.bfloat16)


def maps(lanes):
    return pl.pallas_call(
        maps_kernel,
        out_shape=(
            jax.ShapeDtypeStruct((lanes, 4 * lanes), jnp.bfloat16),
            jax.ShapeDtypeStruct((lanes, 2 * lanes), jnp.bfloat16),
        ),
        out_specs=(pl.BlockSpec(memory_space=pltpu.VMEM),) * 2,
        cost_estimate=pl.CostEstimate(flops=2_000_000_000, bytes_accessed=1_000_000, transcendentals=0),
        compiler_params=pltpu.CompilerParams(vmem_limit_bytes=8 << 20),
        name="maps",
    )()


def matmul(a, b):
    return jnp.dot(a, b, preferred_element_type=jnp.float32)


def two_terms(x):
    high = x.astype(jnp.bfloat16)
    return high, (x - high.astype(jnp.float32)).astype(jnp.bfloat16)


def swept_rows(ext_ref, wind_ref, moved_ref, speed_ref, shift_ref, face_ref, planes):
    count, tall, lanes = ext_ref.shape
    apart = wind_ref.shape[0] // planes - count
    speed_ref[...] = matmul(wind_ref[...].astype(jnp.bfloat16), face_ref[...])
    is_upper = lax.broadcasted_iota(jnp.int32, (tall, lanes), 0) < tall // 2

    def spread(ref, plane, at, columns):
        here, there = (
            jnp.broadcast_to(ref[row : row + 1, columns], (tall, lanes))
            for row in (at * planes + plane, (at + apart) * planes + plane)
        )
        return jnp.where(is_upper, here, there)

    field = [ext_ref[i] for i in range(count)]
    first = 0
    for substep in range(SUB):
        along = [
            spread(wind_ref, 2 * substep, first + i, slice(0, lanes)) for i in range(len(field))
        ]
        speeds = [0.5 * (along[i] + along[i + 1]) for i in range(len(field) - 1)]
        field = sweep_rows(field, speeds)
        first += 2
        size = len(field) * tall
        upper, lower = two_terms(jnp.concatenate(field, 0))
        moved_ref[0:size] = matmul(upper, shift_ref[...]) + matmul(lower, shift_ref[...])
        swept = []
        for i, row in enumerate(field):
            part = slice(i * tall, (i + 1) * tall)
            back2, back1, next1, next2 = (
                moved_ref[part, k * lanes : (k + 1) * lanes] for k in range(4)
            )
            jumps = [back1 - back2, row - back1, next1 - row, next2 - next1]
            slopes = [minmod(jumps[k], jumps[k + 1]) for k in range(3)]
            low_speed, high_speed = (
                spread(speed_ref, 2 * substep + 1, first + i, slice(k * lanes, (k + 1) * lanes))
                for k in range(2)
            )
            low_flux = face_flux(back1, row, slopes[0], slopes[1], jumps[1], low_speed)
            high_flux = face_flux(row, next1, slopes[1], slopes[2], jumps[2], high_speed)
            swept.append(row - (high_flux - low_flux))
        field = swept
    return field


def put(field, out_ref):
    groups = out_ref.shape[1]
    for i, row in enumerate(field):
        out_ref[i] = row[0:groups]
        out_ref[len(field) + i] = row[groups:]


def inner_kernel(own_ref, winds_ref, shift_ref, face_ref, out_ref, ext_ref, wind_ref, moved_ref, speed_ref):
    rows, groups, lanes = own_ref.shape
    planes = winds_ref.shape[1]
    count = ext_ref.shape[0]
    ext_ref[:, 0:groups] = own_ref[0:count]
    ext_ref[:, groups:] = own_ref[rows - count : rows]
    wind_ref[...] = winds_ref[...].astype(jnp.float32).reshape(rows * planes, lanes)
    put(swept_rows(ext_ref, wind_ref, moved_ref, speed_ref, shift_ref, face_ref, planes), out_ref)


def outer_kernel(
    own_ref, winds_ref, above_ref, below_ref, shift_ref, face_ref, out_ref,
    ext_ref, wind_ref, moved_ref, speed_ref,
):
    rows, groups, lanes = own_ref.shape
    planes = winds_ref.shape[1]
    near = 2 * RIM
    above, below = above_ref[...], below_ref[...]
    ext_ref[0:RIM, 0:groups] = above[:, :groups]
    ext_ref[RIM:, 0:groups] = own_ref[0:near]
    ext_ref[0:near, groups:] = own_ref[rows - near : rows]
    ext_ref[near:, groups:] = below[:, :groups]
    rim, block = RIM * planes, near * planes
    wind_ref[0:rim] = above[:, groups:].reshape(rim, lanes)
    wind_ref[rim : rim + block] = winds_ref[0:near].astype(jnp.float32).reshape(block, lanes)
    wind_ref[rim + block : rim + 2 * block] = (
        winds_ref[rows - near : rows].astype(jnp.float32).reshape(block, lanes)
    )
    wind_ref[rim + 2 * block :] = below[:, groups:].reshape(rim, lanes)
    put(swept_rows(ext_ref, wind_ref, moved_ref, speed_ref, shift_ref, face_ref, planes), out_ref)


def sweep_call(kernel, count, depth, flops, own, winds, *others):
    _, groups, lanes = own.shape
    tall, planes = 2 * groups, winds.shape[1]
    return pl.pallas_call(
        kernel,
        out_shape=jax.ShapeDtypeStruct((2 * (count - 2 * RIM), groups, lanes), jnp.float32),
        in_specs=[pl.BlockSpec(memory_space=pltpu.VMEM)] * (2 + len(others)),
        out_specs=pl.BlockSpec(memory_space=pltpu.VMEM),
        scratch_shapes=[
            pltpu.VMEM((count, tall, lanes), jnp.float32),
            pltpu.VMEM((depth * planes, lanes), jnp.float32),
            pltpu.VMEM((count * tall, 4 * lanes), jnp.float32),
            pltpu.VMEM((depth * planes, 2 * lanes), jnp.float32),
        ],
        cost_estimate=pl.CostEstimate(flops=flops, bytes_accessed=600_000, transcendentals=0),
        compiler_params=pltpu.CompilerParams(vmem_limit_bytes=16 << 20),
    )(own, winds, *others)


def tables_kernel(reactants_ref, products_ref, pick_ref, net_ref):
    count = reactants_ref.shape[-1]
    ids = lax.broadcasted_iota(jnp.int32, (S, count), 0)

    def one_hot(ref, place):
        return jnp.where(ids == ref[place : place + 1, :], 1.0, 0.0)

    first, second = one_hot(reactants_ref, 0), one_hot(reactants_ref, 1)
    pick_ref[:, 0:count] = first.astype(jnp.bfloat16)
    pick_ref[:, count:] = second.astype(jnp.bfloat16)
    net = one_hot(products_ref, 0) + one_hot(products_ref, 1) - first - second
    net_ref[...] = net.T.astype(jnp.bfloat16)


def tables(rate_constants, reactants, products):
    count = rate_constants.shape[0]
    made = pl.pallas_call(
        tables_kernel,
        out_shape=(
            jax.ShapeDtypeStruct((S, 2 * count), jnp.bfloat16),
            jax.ShapeDtypeStruct((count, S), jnp.bfloat16),
        ),
        in_specs=[pl.BlockSpec(memory_space=pltpu.VMEM)] * 2,
        out_specs=(pl.BlockSpec(memory_space=pltpu.VMEM),) * 2,
        cost_estimate=pl.CostEstimate(flops=4_000_000_000, bytes_accessed=2_000_000, transcendentals=0),
        compiler_params=pltpu.CompilerParams(vmem_limit_bytes=16 << 20),
        name="tables",
    )(reactants.T, products.T)
    return *made, rate_constants.reshape(1, count)


def chemistry_kernel(cells_ref, pick_ref, net_ref, rate_ref, out_ref):
    count = net_ref.shape[0]
    chunk = 256
    cells = cells_ref[...].reshape(S, cells_ref.shape[-1]).astype(jnp.float32).T

    def picked(cells):
        high, low = two_terms(cells)
        return [
            matmul(high, pick_ref[:, at : at + chunk]) + matmul(low, pick_ref[:, at : at + chunk])
            for at in range(0, 2 * count, chunk)
        ]

    def reacted(cells, found):
        change = jnp.zeros_like(cells)
        for i, at in enumerate(range(0, count, chunk)):
            here = slice(at, at + chunk)
            pair = found[i] * found[i + count // chunk]
            rate_high, rate_low = two_terms(rate_ref[:, here] * pair)
            change = change + matmul(rate_high, net_ref[here]) + matmul(rate_low, net_ref[here])
        return cells + CHEM_STEP * change

    size = cells.shape[0] // 2
    early, late = cells[:size], cells[size:]
    found_late = picked(late)
    for section in range(SECTIONS):
        found_early = picked(early)
        late = reacted(late, found_late)
        early = reacted(early, found_early)
        if section < SECTIONS - 1:
            found_late = picked(late)
    out_ref[...] = jnp.concatenate([early, late], 0).T.reshape(out_ref.shape)


def chemistry(cells, pick, net, rate):
    columns = cells.shape[-1]
    return pl.pallas_call(
        chemistry_kernel,
        out_shape=jax.ShapeDtypeStruct((S, 1, columns), jnp.float32),
        in_specs=[pl.BlockSpec(memory_space=pltpu.VMEM)] * 4,
        out_specs=pl.BlockSpec(memory_space=pltpu.VMEM),
        cost_estimate=pl.CostEstimate(flops=4_000_000_000, bytes_accessed=2_000_000, transcendentals=0),
        compiler_params=pltpu.CompilerParams(vmem_limit_bytes=16 << 20),
        name="chemistry",
    )(cells, pick, net, rate)


def on_device(concentrations, wind_speeds, rate_constants, reactants, products):
    _, _, columns = concentrations.shape
    wide, narrow = lax.axis_size("wide"), lax.axis_size("narrow")
    winds = lax.all_to_all(
        jnp.broadcast_to(wind_speeds[None], (wide, *wind_speeds.shape)), "wide", 0, 0, tiled=True
    ).reshape(wide, SUB * 2, columns)
    moves = maps(columns)
    own = concentrations.swapaxes(0, 1)

    def rim(part):
        return jnp.concatenate([own[part], winds[part].astype(jnp.float32)], 1)

    down = [(i, (i + 1) % narrow) for i in range(narrow)]
    from_above = lax.ppermute(rim(slice(-RIM, None)), "narrow", down)
    from_below = lax.ppermute(rim(slice(RIM)), "narrow", [(j, i) for i, j in down])
    pick, net, rate = tables(rate_constants, reactants, products)
    rows = own.shape[0]
    inner = sweep_call(inner_kernel, rows // 2 + RIM, rows, 4_000_000_000, own, winds, *moves)
    outer = sweep_call(
        outer_kernel, 3 * RIM, 6 * RIM, 1_000_000_000, own, winds, from_above, from_below,
        *moves,
    )
    moved = jnp.concatenate([outer[:RIM], inner, outer[RIM:]], 0)
    cells = lax.all_to_all(moved.astype(SENT), "wide", 0, 0, tiled=True)
    return chemistry(cells.astype(jnp.float32), pick, net, rate)


def solution(mesh):
    return jax.shard_map(
        on_device,
        mesh=mesh,
        in_specs=(
            P("wide", "narrow", None),
            P(None, None, ("narrow", "wide"), None),
            P(),
            P(),
            P(),
        ),
        out_specs=P(None, ("narrow", "wide"), None),
        check_vma=False,
    )
```

```python
import jax
import jax.numpy as jnp
from jax import lax
from jax.experimental import pallas as pl
from jax.experimental.pallas import tpu as pltpu
from jax.sharding import PartitionSpec as P


S = 256
SUB = 2
SECTIONS = 6
DIFFUSION = 0.1
CHEM_STEP = 0.02
RIM = 4
SENT = jnp.float16


def minmod(first_jump, second_jump):
    return jnp.maximum(0.0, jnp.minimum(first_jump, second_jump)) + jnp.minimum(
        0.0, jnp.maximum(first_jump, second_jump)
    )


def face_flux(here, there, slope_here, slope_there, jump, speed):
    forward = speed >= 0.0
    value = jnp.where(forward, here, there)
    slope = jnp.where(forward, slope_here, slope_there)
    reach = jnp.where(forward, 0.5 - 0.5 * speed, -0.5 - 0.5 * speed)
    return speed * (value + reach * slope) - DIFFUSION * jump


def sweep_rows(rows, speeds):
    count = len(rows)
    jumps = [rows[i + 1] - rows[i] for i in range(count - 1)]
    slopes = [None] + [minmod(jumps[i - 1], jumps[i]) for i in range(1, count - 1)]
    fluxes = [None] + [
        face_flux(rows[i], rows[i + 1], slopes[i], slopes[i + 1], jumps[i], speeds[i])
        for i in range(1, count - 2)
    ]
    return [rows[i] - (fluxes[i] - fluxes[i - 1]) for i in range(2, count - 2)]


def maps_kernel(shift_ref, face_ref):
    lanes = shift_ref.shape[0]
    here = lax.broadcasted_iota(jnp.int32, (lanes, lanes), 0)
    there = lax.broadcasted_iota(jnp.int32, (lanes, lanes), 1)
    for i, step in enumerate((-2, -1, 1, 2)):
        moved = jnp.clip(there + step, 0, lanes - 1)
        shift_ref[:, i * lanes : (i + 1) * lanes] = jnp.where(here == moved, 1.0, 0.0).astype(
            jnp.bfloat16
        )
    below = ((here == there) | (here == there - 1)) & (there > 0)
    above = ((here == there) | (here == there + 1)) & (there < lanes - 1)
    face_ref[:, :lanes] = jnp.where(below, 0.5, 0.0).astype(jnp.bfloat16)
    face_ref[:, lanes:] = jnp.where(above, 0.5, 0.0).astype(jnp.bfloat16)


def maps(lanes):
    return pl.pallas_call(
        maps_kernel,
        out_shape=(
            jax.ShapeDtypeStruct((lanes, 4 * lanes), jnp.bfloat16),
            jax.ShapeDtypeStruct((lanes, 2 * lanes), jnp.bfloat16),
        ),
        out_specs=(pl.BlockSpec(memory_space=pltpu.VMEM),) * 2,
        cost_estimate=pl.CostEstimate(flops=2_000_000_000, bytes_accessed=1_000_000, transcendentals=0),
        compiler_params=pltpu.CompilerParams(vmem_limit_bytes=8 << 20),
        name="maps",
    )()


def matmul(a, b):
    return jnp.dot(a, b, preferred_element_type=jnp.float32)


def two_terms(x):
    high = x.astype(jnp.bfloat16)
    return high, (x - high.astype(jnp.float32)).astype(jnp.bfloat16)


def swept_rows(ext_ref, wind_ref, moved_ref, speed_ref, shift_ref, face_ref, planes):
    count, tall, lanes = ext_ref.shape
    apart = wind_ref.shape[0] // planes - count
    speed_ref[...] = matmul(wind_ref[...].astype(jnp.bfloat16), face_ref[...])
    is_upper = lax.broadcasted_iota(jnp.int32, (tall, lanes), 0) < tall // 2

    def spread(ref, plane, at, columns):
        here, there = (
            jnp.broadcast_to(ref[row : row + 1, columns], (tall, lanes))
            for row in (at * planes + plane, (at + apart) * planes + plane)
        )
        return jnp.where(is_upper, here, there)

    field = [ext_ref[i] for i in range(count)]
    first = 0
    for substep in range(SUB):
        along = [
            spread(wind_ref, 2 * substep, first + i, slice(0, lanes)) for i in range(len(field))
        ]
        speeds = [0.5 * (along[i] + along[i + 1]) for i in range(len(field) - 1)]
        field = sweep_rows(field, speeds)
        first += 2
        size = len(field) * tall
        upper, lower = two_terms(jnp.concatenate(field, 0))
        moved_ref[0:size] = matmul(upper, shift_ref[...]) + matmul(lower, shift_ref[...])
        swept = []
        for i, row in enumerate(field):
            part = slice(i * tall, (i + 1) * tall)
            back2, back1, next1, next2 = (
                moved_ref[part, k * lanes : (k + 1) * lanes] for k in range(4)
            )
            jumps = [back1 - back2, row - back1, next1 - row, next2 - next1]
            slopes = [minmod(jumps[k], jumps[k + 1]) for k in range(3)]
            low_speed, high_speed = (
                spread(speed_ref, 2 * substep + 1, first + i, slice(k * lanes, (k + 1) * lanes))
                for k in range(2)
            )
            low_flux = face_flux(back1, row, slopes[0], slopes[1], jumps[1], low_speed)
            high_flux = face_flux(row, next1, slopes[1], slopes[2], jumps[2], high_speed)
            swept.append(row - (high_flux - low_flux))
        field = swept
    return field


def put(field, out_ref):
    groups = out_ref.shape[1]
    for i, row in enumerate(field):
        out_ref[i] = row[0:groups]
        out_ref[len(field) + i] = row[groups:]


def inner_kernel(own_ref, winds_ref, shift_ref, face_ref, out_ref, ext_ref, wind_ref, moved_ref, speed_ref):
    rows, groups, lanes = own_ref.shape
    planes = winds_ref.shape[1]
    count = ext_ref.shape[0]
    ext_ref[:, 0:groups] = own_ref[0:count]
    ext_ref[:, groups:] = own_ref[rows - count : rows]
    wind_ref[...] = winds_ref[...].astype(jnp.float32).reshape(rows * planes, lanes)
    put(swept_rows(ext_ref, wind_ref, moved_ref, speed_ref, shift_ref, face_ref, planes), out_ref)


def outer_kernel(
    own_ref, winds_ref, above_ref, below_ref, shift_ref, face_ref, out_ref,
    ext_ref, wind_ref, moved_ref, speed_ref,
):
    rows, groups, lanes = own_ref.shape
    planes = winds_ref.shape[1]
    near = 2 * RIM
    above, below = above_ref[...], below_ref[...]
    ext_ref[0:RIM, 0:groups] = above[:, :groups]
    ext_ref[RIM:, 0:groups] = own_ref[0:near]
    ext_ref[0:near, groups:] = own_ref[rows - near : rows]
    ext_ref[near:, groups:] = below[:, :groups]
    rim, block = RIM * planes, near * planes
    wind_ref[0:rim] = above[:, groups:].reshape(rim, lanes)
    wind_ref[rim : rim + block] = winds_ref[0:near].astype(jnp.float32).reshape(block, lanes)
    wind_ref[rim + block : rim + 2 * block] = (
        winds_ref[rows - near : rows].astype(jnp.float32).reshape(block, lanes)
    )
    wind_ref[rim + 2 * block :] = below[:, groups:].reshape(rim, lanes)
    put(swept_rows(ext_ref, wind_ref, moved_ref, speed_ref, shift_ref, face_ref, planes), out_ref)


def sweep_call(kernel, count, depth, flops, own, winds, *others):
    _, groups, lanes = own.shape
    tall, planes = 2 * groups, winds.shape[1]
    return pl.pallas_call(
        kernel,
        out_shape=jax.ShapeDtypeStruct((2 * (count - 2 * RIM), groups, lanes), jnp.float32),
        in_specs=[pl.BlockSpec(memory_space=pltpu.VMEM)] * (2 + len(others)),
        out_specs=pl.BlockSpec(memory_space=pltpu.VMEM),
        scratch_shapes=[
            pltpu.VMEM((count, tall, lanes), jnp.float32),
            pltpu.VMEM((depth * planes, lanes), jnp.float32),
            pltpu.VMEM((count * tall, 4 * lanes), jnp.float32),
            pltpu.VMEM((depth * planes, 2 * lanes), jnp.float32),
        ],
        cost_estimate=pl.CostEstimate(flops=flops, bytes_accessed=600_000, transcendentals=0),
        compiler_params=pltpu.CompilerParams(vmem_limit_bytes=16 << 20),
    )(own, winds, *others)


def tables_kernel(reactants_ref, products_ref, pick_ref, net_ref):
    count = reactants_ref.shape[-1]
    ids = lax.broadcasted_iota(jnp.int32, (S, count), 0)

    def one_hot(ref, place):
        return jnp.where(ids == ref[place : place + 1, :], 1.0, 0.0)

    first, second = one_hot(reactants_ref, 0), one_hot(reactants_ref, 1)
    pick_ref[:, 0:count] = first.astype(jnp.bfloat16)
    pick_ref[:, count:] = second.astype(jnp.bfloat16)
    net = one_hot(products_ref, 0) + one_hot(products_ref, 1) - first - second
    net_ref[...] = net.T.astype(jnp.bfloat16)


def tables(rate_constants, reactants, products):
    count = rate_constants.shape[0]
    made = pl.pallas_call(
        tables_kernel,
        out_shape=(
            jax.ShapeDtypeStruct((S, 2 * count), jnp.bfloat16),
            jax.ShapeDtypeStruct((count, S), jnp.bfloat16),
        ),
        in_specs=[pl.BlockSpec(memory_space=pltpu.VMEM)] * 2,
        out_specs=(pl.BlockSpec(memory_space=pltpu.VMEM),) * 2,
        cost_estimate=pl.CostEstimate(flops=4_000_000_000, bytes_accessed=2_000_000, transcendentals=0),
        compiler_params=pltpu.CompilerParams(vmem_limit_bytes=16 << 20),
        name="tables",
    )(reactants.T, products.T)
    return *made, rate_constants.reshape(1, count)


def chemistry_kernel(cells_ref, pick_ref, net_ref, rate_ref, out_ref):
    count = net_ref.shape[0]
    chunk = 256
    cells = cells_ref[...].reshape(S, cells_ref.shape[-1]).astype(jnp.float32).T

    def picked(cells):
        high, low = two_terms(cells)

        def one(at):
            return matmul(high, pick_ref[:, at : at + chunk]) + matmul(low, pick_ref[:, at : at + chunk])

        return [
            rate_ref[:, at : at + chunk] * (one(at) * one(count + at))
            for at in range(0, count, chunk)
        ]

    def reacted(cells, rates, owed, section):
        change = jnp.zeros_like(cells)
        rest = []
        for i, at in enumerate(range(0, count, chunk)):
            rate = rates[i] + owed[i] if section else rates[i]
            high = rate.astype(jnp.bfloat16)
            rest.append(rate - high.astype(jnp.float32))
            net = net_ref[at : at + chunk]
            change = change + matmul(high, net)
            if section == SECTIONS - 1:
                change = change + matmul(rest[i].astype(jnp.bfloat16), net)
        return cells + CHEM_STEP * change, rest

    size = cells.shape[0] // 2
    early, late = cells[:size], cells[size:]
    owed_early = owed_late = None
    rates_late = picked(late)
    for section in range(SECTIONS):
        rates_early = picked(early)
        late, owed_late = reacted(late, rates_late, owed_late, section)
        early, owed_early = reacted(early, rates_early, owed_early, section)
        if section < SECTIONS - 1:
            rates_late = picked(late)
    out_ref[...] = jnp.concatenate([early, late], 0).T.reshape(out_ref.shape)


def chemistry(cells, pick, net, rate):
    columns = cells.shape[-1]
    return pl.pallas_call(
        chemistry_kernel,
        out_shape=jax.ShapeDtypeStruct((S, 1, columns), jnp.float32),
        in_specs=[pl.BlockSpec(memory_space=pltpu.VMEM)] * 4,
        out_specs=pl.BlockSpec(memory_space=pltpu.VMEM),
        cost_estimate=pl.CostEstimate(flops=4_000_000_000, bytes_accessed=2_000_000, transcendentals=0),
        compiler_params=pltpu.CompilerParams(vmem_limit_bytes=16 << 20),
        name="chemistry",
    )(cells, pick, net, rate)


def on_device(concentrations, wind_speeds, rate_constants, reactants, products):
    _, _, columns = concentrations.shape
    wide, narrow = lax.axis_size("wide"), lax.axis_size("narrow")
    winds = lax.all_to_all(
        jnp.broadcast_to(wind_speeds[None], (wide, *wind_speeds.shape)), "wide", 0, 0, tiled=True
    ).reshape(wide, SUB * 2, columns)
    moves = maps(columns)
    own = concentrations.swapaxes(0, 1)

    def rim(part):
        return jnp.concatenate([own[part], winds[part].astype(jnp.float32)], 1)

    down = [(i, (i + 1) % narrow) for i in range(narrow)]
    from_above = lax.ppermute(rim(slice(-RIM, None)), "narrow", down)
    from_below = lax.ppermute(rim(slice(RIM)), "narrow", [(j, i) for i, j in down])
    pick, net, rate = tables(rate_constants, reactants, products)
    rows = own.shape[0]
    inner = sweep_call(inner_kernel, rows // 2 + RIM, rows, 4_000_000_000, own, winds, *moves)
    outer = sweep_call(
        outer_kernel, 3 * RIM, 6 * RIM, 1_000_000_000, own, winds, from_above, from_below,
        *moves,
    )
    moved = jnp.concatenate([outer[:RIM], inner, outer[RIM:]], 0)
    cells = lax.all_to_all(moved.astype(SENT), "wide", 0, 0, tiled=True)
    return chemistry(cells.astype(jnp.float32), pick, net, rate)


def solution(mesh):
    return jax.shard_map(
        on_device,
        mesh=mesh,
        in_specs=(
            P("wide", "narrow", None),
            P(None, None, ("narrow", "wide"), None),
            P(),
            P(),
            P(),
        ),
        out_specs=P(None, ("narrow", "wide"), None),
        check_vma=False,
    )
```
